32 devices in a mesh: front: 4 (over z), tile: 8 (over y, x, core).
Axes of the slice: x: 2, y: 2, z: 4, core: 2. Of those that a mesh axis runs over, the one named last changes fastest.
Arguments:
- lower_basis: bfloat16 [4, 8, 512, 1024], P('front', 'tile'), may hold values from -0.75 to 0.75
- lower_coeff: bfloat16 [4, 8, 512, 1024], P('front', 'tile'), may hold values from -0.75 to 0.75
- upper_basis: bfloat16 [4, 8, 512, 1024], P('front', 'tile'), may hold values from -0.75 to 0.75
- upper_coeff: bfloat16 [4, 8, 512, 1024], P('front', 'tile'), may hold values from -0.75 to 0.75
- lower_rank: int32 [4, 8, 32], P('front', 'tile'), may hold values from 1 to 32
- upper_rank: int32 [4, 8, 32], P('front', 'tile'), may hold values from 1 to 32
- child_half: int32 [4, 8], replicated, may hold values from 0 to 1
- owner_shift: int32 [1, 16], replicated, may hold values from 0 to 3
Outputs:
- parent_tiles: bfloat16 [4, 8, 4096, 512], P('front', 'tile')
The draws below stay inside these ranges and needn't reach their ends.
Inputs may be any that keep to these rules, and one draw needn't show every extreme that they name: `child_half`: 0 keeps a tile's index, 1 moves it by 8.
All inputs are finite; a program needn't handle non-finite values.
Results may differ from the reference program's by a relative error of at most 0.0062.
Values may be sent and summed in bfloat16 or wider, within the bound.
A program may use at most 192 MiB of HBM per device.

```python
import jax
import jax.numpy as jnp
from jax import lax

B = 512
R = 32
KP = 32
K = 1024
NC = 8
PT = 16
FRONTS = 4
PARENTS = 1


def touch_ends(entries, own_key, smallest, top_value):
    dims = entries.shape
    index_at = [jax.random.randint(jax.random.fold_in(own_key, axis), (), 0, dims[axis]) for axis in range(len(dims))]
    entries = entries.at[tuple(index_at)].set(smallest)
    longest = dims.index(max(dims))
    index_at[longest] = (index_at[longest] + 1) % dims[longest]
    return entries.at[tuple(index_at)].set(top_value)


def steps_of(key, extent, pieces, low, largest):
    level = 1.0
    for dim, parts in pieces:
        heights = jax.random.uniform(jax.random.fold_in(jax.random.fold_in(key, 6), dim), (parts,), jnp.float32, low / len(pieces), largest / len(pieces))
        level = level * jnp.repeat(jnp.exp(heights), extent[dim] // parts).reshape((-1,) + (1,) * (len(extent) - 1 - dim))
    return level


def bell_draw(stream_key, extent, deviation, limit, cuts=(), kind=jnp.bfloat16):
    drawn = deviation * jax.random.normal(stream_key, extent, jnp.float32)
    if cuts:
        drawn = drawn * steps_of(stream_key, extent, cuts, -0.22, 0.18)
    return jnp.clip(drawn, -limit, limit).astype(kind)


def setup_inputs(seed: int = 0) -> dict:
    keys = jax.random.split(jax.random.key(seed), 9)
    lower_basis = bell_draw(keys[0], (FRONTS, NC, B, K), ((KP * R * R * B) ** -0.125), 0.75, ((0, 4), (1, 8)))
    lower_coeff = bell_draw(keys[1], (FRONTS, NC, B, K), ((KP * R * R * B) ** -0.125), 0.75, ((0, 4), (1, 8)))
    upper_basis = bell_draw(keys[2], (FRONTS, NC, B, K), ((KP * R * R * B) ** -0.125), 0.75, ((0, 4), (1, 8)))
    upper_coeff = bell_draw(keys[3], (FRONTS, NC, B, K), ((KP * R * R * B) ** -0.125), 0.75, ((0, 4), (1, 8)))
    lower_rank = touch_ends(jax.random.randint(keys[4], (FRONTS, NC, KP), 1, R + 1), jax.random.fold_in(keys[4], 1), 1, R).astype(jnp.int32)
    upper_rank = touch_ends(jax.random.randint(keys[5], (FRONTS, NC, KP), 1, R + 1), jax.random.fold_in(keys[5], 1), 1, R).astype(jnp.int32)
    child_half = touch_ends(jax.random.randint(keys[6], (FRONTS, NC), 0, 2), jax.random.fold_in(keys[6], 1), 0, 1).astype(jnp.int32)
    owner_shift = touch_ends(jax.random.randint(keys[7], (PARENTS, PT), 0, 4), jax.random.fold_in(keys[7], 1), 0, 3).astype(jnp.int32)
    return {"lower_basis": lower_basis, "lower_coeff": lower_coeff, "upper_basis": upper_basis, "upper_coeff": upper_coeff, "lower_rank": lower_rank, "upper_rank": upper_rank, "child_half": child_half, "owner_shift": owner_shift}


def masked(basis, ranks):
    keep = (jnp.arange(R, dtype=jnp.int32)[None, None, :] < ranks[:, :, None]).astype(jnp.float32)
    rows = basis.shape[0]
    return basis.astype(jnp.float32).reshape(rows, B, KP, R) * keep[:, None]


def front_tiles(lower_basis, lower_coeff, upper_basis, upper_coeff, lower_rank, upper_rank):
    lower_kept = masked(lower_basis, lower_rank)
    coeff_rows = lower_coeff.astype(jnp.float32).reshape(NC, B, KP, R)

    def column(packed):
        upper_one, coeff_one, col_ranks = packed
        upper_rows = upper_one.astype(jnp.float32).reshape(B, KP, R)
        upper_kept = masked(coeff_one[None], col_ranks[None])[0].reshape(B, KP * R)
        middle = jnp.einsum('ibkr,bks->ikrs', coeff_rows, upper_rows).astype(jnp.bfloat16)
        middle = lax.optimization_barrier(middle).astype(jnp.float32)
        widened = jnp.einsum('ibkr,ikrs->ibks', lower_kept, middle).astype(jnp.bfloat16)
        widened = lax.optimization_barrier(widened).astype(jnp.float32).reshape(NC, B, KP * R)
        return jnp.einsum('ibk,ck->ibc', widened, upper_kept).astype(jnp.bfloat16)

    return lax.map(column, (upper_basis, upper_coeff, upper_rank))


def reference(lower_basis, lower_coeff, upper_basis, upper_coeff, lower_rank, upper_rank, child_half, owner_shift):
    all_tiles = lax.map(lambda packed: front_tiles(*packed),
                        (lower_basis, lower_coeff, upper_basis, upper_coeff, lower_rank, upper_rank))
    half_rows = NC // 2
    col_ids = jnp.arange(NC, dtype=jnp.int32)[:, None]
    slot_ids = jnp.arange(NC, dtype=jnp.int32)[None, :]
    col_half = slot_ids // half_rows
    row_group = slot_ids % half_rows
    parent_col = col_ids + NC * col_half

    def receiver(out_front):
        parent = out_front // 4
        offset = out_front % 4
        shifts = lax.dynamic_index_in_dim(owner_shift, parent, 0, keepdims=False)
        parent_row = 4 * row_group + (offset - shifts[parent_col]) % 4
        child_row = parent_row % NC
        row_half = parent_row // NC
        assembled = jnp.zeros((NC, NC, B, B), jnp.float32)
        for sibling in range(4):
            child_front = 4 * parent + sibling
            tiles = lax.dynamic_index_in_dim(all_tiles, child_front, 0, keepdims=False)
            halves = lax.dynamic_index_in_dim(child_half, child_front, 0, keepdims=False)
            matches = (halves[col_ids] == col_half) & (halves[child_row] == row_half)
            picked = tiles[col_ids, child_row].astype(jnp.float32)
            assembled = assembled + jnp.where(matches[:, :, None, None], picked, jnp.float32(0.0))
        return assembled.astype(jnp.bfloat16).reshape(NC, NC * B, B)

    return lax.map(receiver, jnp.arange(FRONTS, dtype=jnp.int32))
```

```python
import functools

import jax
import jax.numpy as jnp
from jax import lax
from jax.experimental import pallas as pl
from jax.experimental.pallas import tpu as pltpu
from jax.sharding import PartitionSpec as P

MESH = pl.DeviceIdType.MESH
R = 32
GROUP = 256
CHUNKS = 4
BF16, F32 = jnp.bfloat16, jnp.float32


def expand_ranks(rank_ref, rows, columns):
    col = lax.broadcasted_iota(jnp.int32, (rows, columns), 1)
    panel, within = col // R, col % R
    rank = jnp.zeros((rows, columns), jnp.int32)
    for k in range(columns // R):
        rank = jnp.where(panel == k, rank_ref[0, 0, k], rank)
    return within < rank


def schur_kernel(
    n, xb, yb, pb, qb, lr, ur, half_ref, shift_ref, recv,
    xbuf, ybuf, pbuf, qbuf, ptbuf, mbuf, wbuf, tbuf, zbuf,
    load_sem, send_sem, recv_sem, zsend_sem, zrecv_sem,
):
    block, columns = xb.shape[2:]
    rows = block // CHUNKS
    na = n // 4
    groups = columns // GROUP
    front, me = lax.axis_index("front"), lax.axis_index("tile")
    parent, z = front // 4, lax.rem(front, 4)
    a, b, c = me // 4, lax.rem(me // 2, 2), lax.rem(me, 2)
    first = lax.rem(a, 2) == c
    sib = me + 1 - 2 * c
    across = me + 2 - 4 * b
    peers = [lax.rem(a + d, na) * 4 + b * 2 + c for d in range(1, na)]

    def tile_of(ai, bi, ci):
        return ai * 4 + bi * 2 + ci

    def loads():
        return [
            pltpu.make_async_copy(yb.at[0, 0], ybuf.at[me], load_sem.at[0]),
            pltpu.make_async_copy(xb.at[0, 0], xbuf.at[me], load_sem.at[1]),
            pltpu.make_async_copy(pb.at[0, 0], pbuf, load_sem.at[2]),
            pltpu.make_async_copy(qb.at[0, 0], qbuf, load_sem.at[3]),
        ]

    for copy in loads():
        copy.start()

    barrier = pltpu.get_barrier_semaphore()
    for t in [sib, across] + peers:
        pl.semaphore_signal(barrier, inc=1, device_id={"tile": t}, device_id_type=MESH)
    for d in range(1, 4):
        pl.semaphore_signal(
            barrier, inc=1, device_id={"front": parent * 4 + lax.rem(z + d, 4)},
            device_id_type=MESH,
        )
    pl.semaphore_wait(barrier, 2 + len(peers) + 3)

    def send(kind, is_x, item, ch, target, own=False):
        buf = xbuf if is_x else ybuf
        at = pl.ds(pl.multiple_of(ch * rows, rows), rows)
        src = yb.at[0, 0, at] if own and not is_x else buf.at[item, at]
        s = ch + (CHUNKS if is_x else 0)
        return pltpu.make_async_remote_copy(
            src_ref=src, dst_ref=buf.at[item, at],
            send_sem=send_sem.at[kind, item, s], recv_sem=recv_sem.at[item, s],
            device_id={"tile": target}, device_id_type=MESH,
        )

    def arrived(is_x, item, ch):
        send(0, is_x, item, ch, sib).wait_recv()

    def for_chunks(body):
        def step(ch, carry):
            body(ch)
            return carry
        lax.fori_loop(0, CHUNKS, step, 0)

    def own_first(is_x):
        def body(ch):
            @pl.when(first)
            def _():
                send(1, is_x, me, ch, across, True).start()
            send(0, is_x, me, ch, sib, True).start()
        for_chunks(body)

    def own_rest(is_x):
        def body(ch):
            @pl.when(jnp.logical_not(first))
            def _():
                send(1, is_x, me, ch, across, True).start()
            for d, t in enumerate(peers):
                send(2 + d, is_x, me, ch, t, True).start()
        for_chunks(body)

    own_first(False)
    ycopy, xcopy, pcopy, qcopy = loads()
    xcopy.wait()
    keep = expand_ranks(lr, rows, columns)

    def mask_x(ch):
        at = pl.ds(pl.multiple_of(ch * rows, rows), rows)
        xbuf[me, at] = jnp.where(keep, xbuf[me, at].astype(F32), 0.0).astype(BF16)

    for_chunks(mask_x)
    own_first(True)
    pcopy.wait()
    for g in range(groups):
        at = slice(g * GROUP, (g + 1) * GROUP)
        ptbuf[at, :] = jnp.transpose(pbuf[:, at].astype(F32)).astype(BF16)
    qcopy.wait()
    keep_q = expand_ranks(ur, rows, columns)

    def mask_q(ch):
        at = pl.ds(pl.multiple_of(ch * rows, rows), rows)
        qbuf[at] = jnp.where(keep_q, qbuf[at].astype(F32), 0.0).astype(BF16)

    for_chunks(mask_q)
    ycopy.wait()
    col_half = half_ref[front, me]
    shift = shift_ref[parent, me + n * col_half]

    def base(bi, ci):
        return jnp.where(bi == b, a, ci)

    def zsend(p, d, ch):
        at = pl.ds(pl.multiple_of(ch * rows, rows), rows)
        if d == 0:
            return pltpu.make_async_copy(
                zbuf.at[p, 0, at], recv.at[z, p, at], zsend_sem.at[p, 0, ch]
            )
        return pltpu.make_async_remote_copy(
            src_ref=zbuf.at[p, d, at], dst_ref=recv.at[z, p, at],
            send_sem=zsend_sem.at[p, d, ch], recv_sem=zrecv_sem.at[p, z, ch],
            device_id={"front": parent * 4 + lax.rem(z + d, 4)}, device_id_type=MESH,
        )

    def zarrived(p, d, ch):
        at = pl.ds(pl.multiple_of(ch * rows, rows), rows)
        source = lax.rem(z + d, 4)
        pltpu.make_async_remote_copy(
            src_ref=zbuf.at[p, d, at], dst_ref=recv.at[source, p, at],
            send_sem=zsend_sem.at[p, d, ch], recv_sem=zrecv_sem.at[p, source, ch],
            device_id={"front": parent * 4 + source}, device_id_type=MESH,
        ).wait_recv()

    def relays(p, do):
        near = tile_of(lax.rem(a + p, na), b, c)
        far_a = lax.rem(c + p, na)
        far = tile_of(far_a, 1 - b, c)

        def run(is_x, ch, wait=None):
            if p > 0:
                if wait:
                    wait(is_x, near, ch)
                do(0, is_x, near, ch, sib)
                if na == 2:
                    @pl.when(lax.rem(a + p, 2) != c)
                    def _():
                        do(1, is_x, near, ch, across)
            if wait:
                wait(is_x, far, ch)

            @pl.when(far_a == a if na > 2 else jnp.logical_and(far_a == a, first))
            def _():
                for d, t in enumerate(peers):
                    do(2 + d, is_x, far, ch, t)
            do(0, is_x, far, ch, sib)

        return run

    def do_start(kind, is_x, item, ch, target):
        send(kind, is_x, item, ch, target).start()

    def do_wait(kind, is_x, item, ch, target):
        send(kind, is_x, item, ch, target).wait_send()

    row = lax.broadcasted_iota(jnp.int32, (GROUP, GROUP), 0) // R
    col = lax.broadcasted_iota(jnp.int32, (GROUP, GROUP), 1) // R
    diagonal = row == col

    for p in range(na):
        forward = relays(p, do_start)
        items = [
            tile_of(lax.rem(base(rr // 2, rr % 2) + p, na), rr // 2, rr % 2)
            for rr in range(4)
        ]
        sib_near = tile_of(lax.rem(a + p, na), b, 1 - c)
        sib_far = tile_of(lax.rem(1 - c + p, na), 1 - b, 1 - c)

        def take(is_x, ch):
            forward(is_x, ch, arrived)

        for_chunks(lambda ch: take(False, ch))

        def sib_y(ch):
            arrived(False, sib_near, ch)
            arrived(False, sib_far, ch)

        for_chunks(sib_y)
        for rr in range(4):
            for g in range(groups):
                at = slice(g * GROUP, (g + 1) * GROUP)
                middle = jnp.dot(
                    ptbuf[at, :], ybuf[items[rr], :, at], preferred_element_type=F32
                )
                mbuf[rr, g] = jnp.where(diagonal, middle, 0.0).astype(BF16)

        def step(ch):
            take(True, ch)
            arrived(True, sib_near, ch)
            arrived(True, sib_far, ch)
            at = pl.ds(pl.multiple_of(ch * rows, rows), rows)
            for rr in range(4):
                for g in range(groups):
                    cols = slice(g * GROUP, (g + 1) * GROUP)
                    wbuf[rr * rows:(rr + 1) * rows, cols] = lax.dot_general(
                        xbuf[items[rr], at, cols], mbuf[rr, g],
                        (((1,), (1,)), ((), ())), preferred_element_type=F32,
                    ).astype(BF16)
            for rr in range(4):
                tbuf[rr] = lax.dot_general(
                    wbuf[rr * rows:(rr + 1) * rows, :], qbuf[...],
                    (((1,), (1,)), ((), ())), preferred_element_type=F32,
                ).astype(BF16)
            for d in range(4):
                residue = lax.rem(z + d - shift + 4, 4)
                zbuf[p, d, at] = tbuf[residue]
            for d in (2, 3, 1, 0):
                zsend(p, d, ch).start()
            if p == 0:
                @pl.when(ch == 0)
                def _():
                    own_rest(False)
                    own_rest(True)

        for_chunks(step)

    def drain(ch):
        for is_x in (False, True):
            send(0, is_x, me, ch, sib, True).wait_send()
            send(1, is_x, me, ch, across, True).wait_send()
            for d, t in enumerate(peers):
                send(2 + d, is_x, me, ch, t, True).wait_send()
            for p in range(na):
                relays(p, do_wait)(is_x, ch)

    for_chunks(drain)

    def zdrain(ch):
        for p in range(na):
            zsend(p, 0, ch).wait()
            for d in range(1, 4):
                zsend(p, d, ch).wait_send()
            for d in range(1, 4):
                zarrived(p, d, ch)

    for_chunks(zdrain)


def assemble_kernel(n, half_ref, shift_ref, recv, out):
    na = n // 4
    front, me = lax.axis_index("front"), lax.axis_index("tile")
    parent, z = front // 4, lax.rem(front, 4)
    a, b = me // 4, lax.rem(me // 2, 2)
    source = []
    for s in range(4):
        child = 4 * parent + s
        col_half = half_ref[child, me]
        residue = lax.rem(z - shift_ref[parent, me + n * col_half] + 4, 4)
        start = jnp.where(residue // 2 == b, a, lax.rem(residue, 2))
        source.append((child, col_half, residue, start))
    for q in range(na):
        picked = []
        for s, (child, col_half, residue, start) in enumerate(source):
            p = lax.rem(q - start + na, na)
            picked.append((recv[s, p], col_half * 2 + half_ref[child, 4 * q + residue]))
        for halves in range(4):
            total = jnp.zeros(out.shape[1:], F32)
            for tile, own in picked:
                total = total + jnp.where(own == halves, tile.astype(F32), 0.0)
            slot = (halves // 2) * (n // 2) + (halves % 2) * na + q
            out[slot] = total.astype(out.dtype)


def solution(mesh):
    n = mesh.shape["tile"]
    na = n // 4

    def per_device(xb, yb, pb, qb, lr, ur, half, shift):
        block, columns = xb.shape[2:]
        rows = block // CHUNKS
        anywhere = pl.BlockSpec(memory_space=pl.ANY)
        scalars = pl.BlockSpec(memory_space=pltpu.SMEM)
        received = pl.pallas_call(
            functools.partial(schur_kernel, n),
            out_shape=jax.ShapeDtypeStruct((4, na, block, block), BF16),
            in_specs=[anywhere] * 4 + [scalars] * 4,
            out_specs=anywhere,
            scratch_shapes=[
                pltpu.VMEM((n, block, columns), BF16),
                pltpu.VMEM((n, block, columns), BF16),
                pltpu.VMEM((block, columns), BF16),
                pltpu.VMEM((block, columns), BF16),
                pltpu.VMEM((columns, block), BF16),
                pltpu.VMEM((4, columns // GROUP, GROUP, GROUP), BF16),
                pltpu.VMEM((4 * rows, columns), BF16),
                pltpu.VMEM((4, rows, block), BF16),
                pltpu.VMEM((na, 4, block, block), BF16),
                pltpu.SemaphoreType.DMA((4,)),
                pltpu.SemaphoreType.DMA((na + 1, n, 2 * CHUNKS)),
                pltpu.SemaphoreType.DMA((n, 2 * CHUNKS)),
                pltpu.SemaphoreType.DMA((na, 4, CHUNKS)),
                pltpu.SemaphoreType.DMA((na, 4, CHUNKS)),
            ],
            compiler_params=pltpu.CompilerParams(
                collective_id=0, has_side_effects=True, vmem_limit_bytes=60 * 2**20
            ),
        )(xb, yb, pb, qb, lr, ur, half, shift)
        strip = 64
        out = pl.pallas_call(
            functools.partial(assemble_kernel, n),
            grid=(block // strip,),
            out_shape=jax.ShapeDtypeStruct((n, block, block), BF16),
            in_specs=[scalars, scalars,
                      pl.BlockSpec((4, na, strip, block), lambda r: (0, 0, r, 0))],
            out_specs=pl.BlockSpec((n, strip, block), lambda r: (0, r, 0)),
        )(half, shift, received)
        return out.reshape(1, 1, n * block, block)

    split = P("front", "tile", None, None)
    ranks = P("front", "tile", None)
    return jax.shard_map(
        per_device, mesh=mesh,
        in_specs=(split, split, split, split, ranks, ranks, P(), P()),
        out_specs=split, check_vma=False,
    )
```

```python
import functools

import jax
import jax.numpy as jnp
from jax import lax
from jax.experimental import pallas as pl
from jax.experimental.pallas import tpu as pltpu
from jax.sharding import PartitionSpec as P

MESH = pl.DeviceIdType.MESH
R = 32
GROUP = 256
CHUNKS = 2
WINDOW = 2
BF16, F32 = jnp.bfloat16, jnp.float32


def expand_ranks(rank_ref, rows, columns):
    col = lax.broadcasted_iota(jnp.int32, (rows, columns), 1)
    panel, within = col // R, col % R
    rank = jnp.zeros((rows, columns), jnp.int32)
    for k in range(columns // R):
        rank = jnp.where(panel == k, rank_ref[0, 0, k], rank)
    return within < rank


def schur_kernel(
    n, xb, yb, pb, qb, lr, ur, half_ref, shift_ref, recv,
    xbuf, ybuf, pbuf, qbuf, ptbuf, mbuf, wbuf, tbuf, zbuf,
    load_sem, send_sem, recv_sem, zsend_sem, zrecv_sem,
):
    block, columns = xb.shape[2:]
    rows = block // CHUNKS
    na = n // 4
    groups = columns // GROUP
    front, me = lax.axis_index("front"), lax.axis_index("tile")
    parent, z = front // 4, lax.rem(front, 4)
    a, b, c = me // 4, lax.rem(me // 2, 2), lax.rem(me, 2)
    turn = lax.rem(a - c + na, na)
    sib = me + 1 - 2 * c
    across = me + 2 - 4 * b
    peers = [lax.rem(a - d + na, na) * 4 + b * 2 + c for d in range(1, na)]

    def tile_of(ai, bi, ci):
        return ai * 4 + bi * 2 + ci

    def loads():
        return [
            pltpu.make_async_copy(yb.at[0, 0], ybuf.at[me], load_sem.at[0]),
            pltpu.make_async_copy(xb.at[0, 0], xbuf.at[me], load_sem.at[1]),
            pltpu.make_async_copy(pb.at[0, 0], pbuf, load_sem.at[2]),
            pltpu.make_async_copy(qb.at[0, 0], qbuf, load_sem.at[3]),
        ]

    for copy in loads():
        copy.start()

    barrier = pltpu.get_barrier_semaphore()
    for t in [sib, across] + peers:
        pl.semaphore_signal(barrier, inc=1, device_id={"tile": t}, device_id_type=MESH)
    for d in range(1, 4):
        pl.semaphore_signal(
            barrier, inc=1, device_id={"front": parent * 4 + lax.rem(z + d, 4)},
            device_id_type=MESH,
        )
    pl.semaphore_wait(barrier, 2 + len(peers) + 3)

    def send(kind, is_x, item, ch, target, own=False):
        buf = xbuf if is_x else ybuf
        at = pl.ds(pl.multiple_of(ch * rows, rows), rows)
        src = yb.at[0, 0, at] if own and not is_x else buf.at[item, at]
        s = ch + (CHUNKS if is_x else 0)
        return pltpu.make_async_remote_copy(
            src_ref=src, dst_ref=buf.at[item, at],
            send_sem=send_sem.at[kind, item, s], recv_sem=recv_sem.at[item, s],
            device_id={"tile": target}, device_id_type=MESH,
        )

    def arrived(is_x, item, ch):
        send(0, is_x, item, ch, sib).wait_recv()

    def for_chunks(body):
        def step(ch, carry):
            body(ch)
            return carry
        lax.fori_loop(0, CHUNKS, step, 0)

    def own_copies(p, is_x, ch, do):
        @pl.when(turn == p)
        def _():
            do(send(1, is_x, me, ch, across, True))
        if p > 0:
            do(send(1 + p, is_x, me, ch, peers[p - 1], True))

    def start(copy):
        copy.start()

    def own_ahead(p, is_x, ch):
        @pl.when(ch < CHUNKS - WINDOW)
        def _():
            own_copies(p, is_x, ch + WINDOW, start)

        p_next = p + 1 if is_x else p
        if p_next < na:
            @pl.when(ch >= CHUNKS - WINDOW)
            def _():
                own_copies(p_next, not is_x, ch + WINDOW - CHUNKS, start)

    for ch in range(WINDOW):
        own_copies(0, False, ch, start)
    for_chunks(lambda ch: send(0, False, me, ch, sib, True).start())
    ycopy, xcopy, pcopy, qcopy = loads()
    xcopy.wait()
    keep = expand_ranks(lr, rows, columns)

    def mask_x(ch):
        at = pl.ds(pl.multiple_of(ch * rows, rows), rows)
        xbuf[me, at] = jnp.where(keep, xbuf[me, at].astype(F32), 0.0).astype(BF16)

    for_chunks(mask_x)
    for_chunks(lambda ch: send(0, True, me, ch, sib, True).start())
    pcopy.wait()
    for g in range(groups):
        at = slice(g * GROUP, (g + 1) * GROUP)
        ptbuf[at, :] = jnp.transpose(pbuf[:, at].astype(F32)).astype(BF16)
    qcopy.wait()
    keep_q = expand_ranks(ur, rows, columns)

    def mask_q(ch):
        at = pl.ds(pl.multiple_of(ch * rows, rows), rows)
        qbuf[at] = jnp.where(keep_q, qbuf[at].astype(F32), 0.0).astype(BF16)

    for_chunks(mask_q)
    ycopy.wait()
    col_half = half_ref[front, me]
    shift = shift_ref[parent, me + n * col_half]

    def base(bi, ci):
        return jnp.where(bi == b, a, ci)

    def zsend(p, d, ch):
        at = pl.ds(pl.multiple_of(ch * rows, rows), rows)
        if d == 0:
            return pltpu.make_async_copy(
                zbuf.at[p, 0, at], recv.at[z, p, at], zsend_sem.at[p, 0, ch]
            )
        return pltpu.make_async_remote_copy(
            src_ref=zbuf.at[p, d, at], dst_ref=recv.at[z, p, at],
            send_sem=zsend_sem.at[p, d, ch], recv_sem=zrecv_sem.at[p, z, ch],
            device_id={"front": parent * 4 + lax.rem(z + d, 4)}, device_id_type=MESH,
        )

    def zarrived(p, d, ch):
        at = pl.ds(pl.multiple_of(ch * rows, rows), rows)
        source = lax.rem(z + d, 4)
        pltpu.make_async_remote_copy(
            src_ref=zbuf.at[p, d, at], dst_ref=recv.at[source, p, at],
            send_sem=zsend_sem.at[p, d, ch], recv_sem=zrecv_sem.at[p, source, ch],
            device_id={"front": parent * 4 + source}, device_id_type=MESH,
        ).wait_recv()

    def relays(p, do):
        near = tile_of(lax.rem(a + p, na), b, c)
        far_a = lax.rem(c + p, na)
        far = tile_of(far_a, 1 - b, c)

        def run(is_x, ch, wait=None):
            if p > 0:
                if wait:
                    wait(is_x, near, ch)
                if na == 2:
                    @pl.when(lax.rem(a + p, 2) != c)
                    def _():
                        do(1, is_x, near, ch, across)
                do(0, is_x, near, ch, sib)
            if wait:
                wait(is_x, far, ch)

            if na > 2 or p == 0:
                @pl.when(far_a == a)
                def _():
                    for d, t in enumerate(peers):
                        do(2 + d, is_x, far, ch, t)
            do(0, is_x, far, ch, sib)

        return run

    def do_start(kind, is_x, item, ch, target):
        send(kind, is_x, item, ch, target).start()

    def do_wait(kind, is_x, item, ch, target):
        send(kind, is_x, item, ch, target).wait_send()

    row = lax.broadcasted_iota(jnp.int32, (GROUP, GROUP), 0) // R
    col = lax.broadcasted_iota(jnp.int32, (GROUP, GROUP), 1) // R
    diagonal = row == col

    for p in range(na):
        forward = relays(p, do_start)
        items = [
            tile_of(lax.rem(base(rr // 2, rr % 2) + p, na), rr // 2, rr % 2)
            for rr in range(4)
        ]
        sib_near = tile_of(lax.rem(a + p, na), b, 1 - c)
        sib_far = tile_of(lax.rem(1 - c + p, na), 1 - b, 1 - c)

        def take(is_x, ch):
            forward(is_x, ch, arrived)
            own_ahead(p, is_x, ch)

        for_chunks(lambda ch: take(False, ch))

        def sib_y(ch):
            arrived(False, sib_near, ch)
            arrived(False, sib_far, ch)

        for_chunks(sib_y)
        for rr in range(4):
            for g in range(groups):
                at = slice(g * GROUP, (g + 1) * GROUP)
                middle = jnp.dot(
                    ptbuf[at, :], ybuf[items[rr], :, at], preferred_element_type=F32
                )
                mbuf[rr, g] = jnp.where(diagonal, middle, 0.0).astype(BF16)

        def step(ch):
            take(True, ch)
            arrived(True, sib_near, ch)
            arrived(True, sib_far, ch)
            at = pl.ds(pl.multiple_of(ch * rows, rows), rows)
            for rr in range(4):
                for g in range(groups):
                    cols = slice(g * GROUP, (g + 1) * GROUP)
                    wbuf[rr * rows:(rr + 1) * rows, cols] = lax.dot_general(
                        xbuf[items[rr], at, cols], mbuf[rr, g],
                        (((1,), (1,)), ((), ())), preferred_element_type=F32,
                    ).astype(BF16)
            for rr in range(4):
                tbuf[rr] = lax.dot_general(
                    wbuf[rr * rows:(rr + 1) * rows, :], qbuf[...],
                    (((1,), (1,)), ((), ())), preferred_element_type=F32,
                ).astype(BF16)
            for d in range(4):
                residue = lax.rem(z + d - shift + 4, 4)
                zbuf[p, d, at] = tbuf[residue]
            for d in (2, 3, 1, 0):
                zsend(p, d, ch).start()

        for_chunks(step)

    def drain(ch):
        for is_x in (False, True):
            send(0, is_x, me, ch, sib, True).wait_send()
            for p in range(na):
                own_copies(p, is_x, ch, lambda copy: copy.wait_send())
            for p in range(na):
                relays(p, do_wait)(is_x, ch)

    for_chunks(drain)

    def zdrain(ch):
        for p in range(na):
            zsend(p, 0, ch).wait()
            for d in range(1, 4):
                zsend(p, d, ch).wait_send()
            for d in range(1, 4):
                zarrived(p, d, ch)

    for_chunks(zdrain)


def assemble_kernel(n, half_ref, shift_ref, recv, out):
    na = n // 4
    front, me = lax.axis_index("front"), lax.axis_index("tile")
    parent, z = front // 4, lax.rem(front, 4)
    a, b = me // 4, lax.rem(me // 2, 2)
    source = []
    for s in range(4):
        child = 4 * parent + s
        col_half = half_ref[child, me]
        residue = lax.rem(z - shift_ref[parent, me + n * col_half] + 4, 4)
        start = jnp.where(residue // 2 == b, a, lax.rem(residue, 2))
        source.append((child, col_half, residue, start))
    for q in range(na):
        picked = []
        for s, (child, col_half, residue, start) in enumerate(source):
            p = lax.rem(q - start + na, na)
            picked.append((recv[s, p], col_half * 2 + half_ref[child, 4 * q + residue]))
        for halves in range(4):
            total = jnp.zeros(out.shape[1:], F32)
            for tile, own in picked:
                total = total + jnp.where(own == halves, tile.astype(F32), 0.0)
            slot = (halves // 2) * (n // 2) + (halves % 2) * na + q
            out[slot] = total.astype(out.dtype)


def solution(mesh):
    n = mesh.shape["tile"]
    na = n // 4

    def per_device(xb, yb, pb, qb, lr, ur, half, shift):
        block, columns = xb.shape[2:]
        rows = block // CHUNKS
        anywhere = pl.BlockSpec(memory_space=pl.ANY)
        scalars = pl.BlockSpec(memory_space=pltpu.SMEM)
        received = pl.pallas_call(
            functools.partial(schur_kernel, n),
            out_shape=jax.ShapeDtypeStruct((4, na, block, block), BF16),
            in_specs=[anywhere] * 4 + [scalars] * 4,
            out_specs=anywhere,
            scratch_shapes=[
                pltpu.VMEM((n, block, columns), BF16),
                pltpu.VMEM((n, block, columns), BF16),
                pltpu.VMEM((block, columns), BF16),
                pltpu.VMEM((block, columns), BF16),
                pltpu.VMEM((columns, block), BF16),
                pltpu.VMEM((4, columns // GROUP, GROUP, GROUP), BF16),
                pltpu.VMEM((4 * rows, columns), BF16),
                pltpu.VMEM((4, rows, block), BF16),
                pltpu.VMEM((na, 4, block, block), BF16),
                pltpu.SemaphoreType.DMA((4,)),
                pltpu.SemaphoreType.DMA((na + 1, n, 2 * CHUNKS)),
                pltpu.SemaphoreType.DMA((n, 2 * CHUNKS)),
                pltpu.SemaphoreType.DMA((na, 4, CHUNKS)),
                pltpu.SemaphoreType.DMA((na, 4, CHUNKS)),
            ],
            compiler_params=pltpu.CompilerParams(
                collective_id=0, has_side_effects=True, vmem_limit_bytes=60 * 2**20
            ),
        )(xb, yb, pb, qb, lr, ur, half, shift)
        strip = 128
        out = pl.pallas_call(
            functools.partial(assemble_kernel, n),
            grid=(block // strip,),
            out_shape=jax.ShapeDtypeStruct((n, block, block), BF16),
            in_specs=[scalars, scalars,
                      pl.BlockSpec((4, na, strip, block), lambda r: (0, 0, r, 0))],
            out_specs=pl.BlockSpec((n, strip, block), lambda r: (0, r, 0)),
        )(half, shift, received)
        return out.reshape(1, 1, n * block, block)

    split = P("front", "tile", None, None)
    ranks = P("front", "tile", None)
    return jax.shard_map(
        per_device, mesh=mesh,
        in_specs=(split, split, split, split, ranks, ranks, P(), P()),
        out_specs=split, check_vma=False,
    )
```
